8 devices in a mesh: dp: 2 (over z, y), ep: 4 (over x, core).
Axes of the slice: x: 2, y: 2, z: 1, core: 2. Of those that a mesh axis runs over, the one named last changes fastest.
Arguments:
- tok_x: bfloat16 [8192, 4096], P(('dp', 'ep'))
- tok_dy: bfloat16 [8192, 4096], P(('dp', 'ep'))
- exp_first: int32 [8192], P(('dp', 'ep'))
- exp_second: int32 [8192], P(('dp', 'ep'))
- eligible: int32 [8192, 8], P(('dp', 'ep'))
- slot_first: int32 [8192], P(('dp', 'ep'))
- slot_second: int32 [8192], P(('dp', 'ep'))
- ln_weight: bfloat16 [4096], replicated
- ln_bias: bfloat16 [4096], replicated
- router: bfloat16 [4096, 8], replicated
- w_gate: bfloat16 [8, 4096, 1376], P('ep')
- w_up: bfloat16 [8, 4096, 1376], P('ep')
- w_down: bfloat16 [8, 1376, 4096], P('ep')
Outputs:
- output 1: bfloat16 [8192, 4096], P(('dp', 'ep'))
- output 2: bfloat16 [8192, 4096], P(('dp', 'ep'))
- output 3: float32 [8, 4096, 1376], P('ep')
- output 4: float32 [8, 4096, 1376], P('ep')
- output 5: float32 [8, 1376, 4096], P('ep')
- output 6: float32 [4096, 8], replicated
- output 7: float32 [4096], replicated
- output 8: float32 [4096], replicated
All inputs are finite; a program needn't handle non-finite values.
Results may differ from the reference program's by a relative error of at most 0.00492321.
Values are sent between devices in bfloat16 or wider.
A program may use at most 1 GiB of HBM per device.

```python
import jax
import jax.numpy as jnp
from jax import lax

SHARDS = 8
TOK_DEV = 1024
D_MODEL = 4096
FF_DIM = 1376
EXPERTS = 8
SLOT_CAP = 384
LN_EPS = 1e-5


def draw_routing(rng_key):
    n_tok = SHARDS * TOK_DEV
    key_list = jax.random.split(rng_key, 5)
    pick_a = jax.random.randint(key_list[0], (n_tok,), 0, EXPERTS)
    pick_b = jax.random.randint(key_list[1], (n_tok,), 0, EXPERTS)
    pick_c = jax.random.randint(key_list[2], (n_tok,), 0, EXPERTS)
    first_pick = jnp.minimum(jnp.minimum(pick_a, pick_b), pick_c)
    second_pick = (first_pick + 1 + jax.random.randint(key_list[3], (n_tok,), 0, EXPERTS - 1)) % EXPERTS
    expert_ids = jnp.arange(EXPERTS)
    hot_first = (first_pick[:, None] == expert_ids[None, :]).astype(jnp.int32)
    hot_second = (second_pick[:, None] == expert_ids[None, :]).astype(jnp.int32)
    extra_bits = (jax.random.randint(key_list[4], (n_tok, EXPERTS), 0, 8) == 0).astype(jnp.int32)
    eligible = jnp.maximum(extra_bits, jnp.maximum(hot_first, hot_second))
    per_first = hot_first.reshape(SHARDS, TOK_DEV, EXPERTS)
    per_second = hot_second.reshape(SHARDS, TOK_DEV, EXPERTS)
    rank_first = jnp.sum((jnp.cumsum(per_first, axis=1) - per_first) * per_first, axis=2).reshape(n_tok)
    used_first = jnp.sum(per_first, axis=1, keepdims=True)
    rank_second = jnp.sum((jnp.cumsum(per_second, axis=1) - per_second + used_first) * per_second, axis=2).reshape(n_tok)
    slot_first = jnp.where(rank_first < SLOT_CAP, rank_first, -1)
    slot_second = jnp.where(rank_second < SLOT_CAP, rank_second, -1)
    return first_pick, second_pick, eligible, slot_first, slot_second


def setup_inputs(seed: int = 0) -> dict:
    key_list = jax.random.split(jax.random.key(seed), 10)
    n_tok = SHARDS * TOK_DEV
    first_pick, second_pick, eligible, slot_first, slot_second = draw_routing(key_list[0])
    tok_x = jax.random.normal(key_list[1], (n_tok, D_MODEL), jnp.float32).astype(jnp.bfloat16)
    tok_dy = jax.random.normal(key_list[2], (n_tok, D_MODEL), jnp.float32).astype(jnp.bfloat16)
    ln_weight = (1.0 + 0.3 * jax.random.normal(key_list[3], (D_MODEL,), jnp.float32)).astype(jnp.bfloat16)
    ln_bias = (0.3 * jax.random.normal(key_list[4], (D_MODEL,), jnp.float32)).astype(jnp.bfloat16)
    router = (1.5 * D_MODEL ** -0.5 * jax.random.normal(key_list[5], (D_MODEL, EXPERTS), jnp.float32)).astype(jnp.bfloat16)
    w_gate = (D_MODEL ** -0.5 * jax.random.normal(key_list[6], (EXPERTS, D_MODEL, FF_DIM), jnp.float32)).astype(jnp.bfloat16)
    w_up = (D_MODEL ** -0.5 * jax.random.normal(key_list[7], (EXPERTS, D_MODEL, FF_DIM), jnp.float32)).astype(jnp.bfloat16)
    w_down = (3.0 * FF_DIM ** -0.5 * jax.random.normal(key_list[8], (EXPERTS, FF_DIM, D_MODEL), jnp.float32)).astype(jnp.bfloat16)
    return {'tok_x': tok_x, 'tok_dy': tok_dy, 'exp_first': first_pick, 'exp_second': second_pick,
            'eligible': eligible, 'slot_first': slot_first, 'slot_second': slot_second,
            'ln_weight': ln_weight, 'ln_bias': ln_bias, 'router': router,
            'w_gate': w_gate, 'w_up': w_up, 'w_down': w_down}


def layer_norm(x_rows, ln_weight, ln_bias):
    x_float = x_rows.astype(jnp.float32)
    centered = x_float - jnp.mean(x_float, axis=-1, keepdims=True)
    inv_std = lax.rsqrt(jnp.mean(centered * centered, axis=-1, keepdims=True) + LN_EPS)
    x_hat = centered * inv_std
    hidden = (x_hat * ln_weight.astype(jnp.float32) + ln_bias.astype(jnp.float32)).astype(jnp.bfloat16)
    return hidden, x_hat, inv_std


def layer_norm_back(grad_h, x_hat, inv_std, ln_weight):
    scaled = grad_h * ln_weight.astype(jnp.float32)
    return inv_std * (scaled - jnp.mean(scaled, axis=-1, keepdims=True)
                      - x_hat * jnp.mean(scaled * x_hat, axis=-1, keepdims=True))


def masked_gate(logits, allowed, choice):
    expert_ids = jnp.arange(logits.shape[-1])
    prob_all = jax.nn.softmax(jnp.where(allowed, logits, -1e30), axis=-1)
    picked = (choice[:, None] == expert_ids[None, :]).astype(jnp.float32)
    return jnp.sum(prob_all * picked, axis=-1), prob_all, picked


def expert_pass(operands):
    hid_rows, grad_rows, gate_w, up_w, down_w = operands
    pre_gate = jnp.dot(hid_rows, gate_w, preferred_element_type=jnp.float32)
    pre_up = jnp.dot(hid_rows, up_w, preferred_element_type=jnp.float32)
    sig_gate = jax.nn.sigmoid(pre_gate)
    silu_gate = pre_gate * sig_gate
    inner_act = (silu_gate * pre_up).astype(jnp.bfloat16)
    exp_out = jnp.dot(inner_act, down_w, preferred_element_type=jnp.float32).astype(jnp.bfloat16)
    grad_inner = jnp.dot(grad_rows, down_w.T, preferred_element_type=jnp.float32)
    grad_pre_gate = (grad_inner * pre_up * sig_gate * (1.0 + pre_gate * (1.0 - sig_gate))).astype(jnp.bfloat16)
    grad_pre_up = (grad_inner * silu_gate).astype(jnp.bfloat16)
    grad_hid = (jnp.dot(grad_pre_gate, gate_w.T, preferred_element_type=jnp.float32)
                + jnp.dot(grad_pre_up, up_w.T, preferred_element_type=jnp.float32)).astype(jnp.bfloat16)
    dw_gate = jnp.dot(hid_rows.T, grad_pre_gate, preferred_element_type=jnp.float32)
    dw_up = jnp.dot(hid_rows.T, grad_pre_up, preferred_element_type=jnp.float32)
    dw_down = jnp.dot(inner_act.T, grad_rows, preferred_element_type=jnp.float32)
    return exp_out, grad_hid, dw_gate, dw_up, dw_down


def reference(tok_x, tok_dy, exp_first, exp_second, eligible, slot_first, slot_second,
              ln_weight, ln_bias, router, w_gate, w_up, w_down):
    n_tok = tok_x.shape[0]
    hidden, x_hat, inv_std = layer_norm(tok_x, ln_weight, ln_bias)
    logits = jnp.dot(hidden, router, preferred_element_type=jnp.float32)
    expert_ids = jnp.arange(EXPERTS)
    allowed = eligible > 0
    gate_one, prob_one, pick_one = masked_gate(logits, allowed, exp_first)
    gate_two, prob_two, pick_two = masked_gate(logits, allowed & (expert_ids[None, :] != exp_first[:, None]), exp_second)
    n_rows = EXPERTS * SHARDS * SLOT_CAP
    shard_idx = jnp.arange(n_tok) // TOK_DEV
    row_one = jnp.where(slot_first >= 0, (exp_first * SHARDS + shard_idx) * SLOT_CAP + slot_first, n_rows)
    row_two = jnp.where(slot_second >= 0, (exp_second * SHARDS + shard_idx) * SLOT_CAP + slot_second, n_rows)
    dy_float = tok_dy.astype(jnp.float32)
    grad_one = (gate_one[:, None] * dy_float).astype(jnp.bfloat16)
    grad_two = (gate_two[:, None] * dy_float).astype(jnp.bfloat16)
    empty_rows = jnp.zeros((n_rows, D_MODEL), jnp.bfloat16)
    hid_buf = empty_rows.at[row_one].set(hidden, mode='drop').at[row_two].set(hidden, mode='drop')
    grad_buf = empty_rows.at[row_one].set(grad_one, mode='drop').at[row_two].set(grad_two, mode='drop')
    exp_out, grad_hid, dw_gate, dw_up, dw_down = lax.map(
        expert_pass,
        (hid_buf.reshape(EXPERTS, SHARDS * SLOT_CAP, D_MODEL), grad_buf.reshape(EXPERTS, SHARDS * SLOT_CAP, D_MODEL),
         w_gate, w_up, w_down))
    exp_out = exp_out.reshape(n_rows, D_MODEL)
    grad_hid = grad_hid.reshape(n_rows, D_MODEL)
    out_one = jnp.take(exp_out, row_one, axis=0, mode='fill', fill_value=0).astype(jnp.float32)
    out_two = jnp.take(exp_out, row_two, axis=0, mode='fill', fill_value=0).astype(jnp.float32)
    y_mix = gate_one[:, None] * out_one + gate_two[:, None] * out_two
    out_tok = (tok_x.astype(jnp.float32) + y_mix).astype(jnp.bfloat16)
    dgate_one = jnp.sum(dy_float * out_one, axis=-1)
    dgate_two = jnp.sum(dy_float * out_two, axis=-1)
    d_logits = ((dgate_one * gate_one)[:, None] * (pick_one - prob_one)
                + (dgate_two * gate_two)[:, None] * (pick_two - prob_two)).astype(jnp.bfloat16)
    d_router = jnp.dot(hidden.T, d_logits, preferred_element_type=jnp.float32)
    grad_h = (jnp.dot(d_logits, router.T, preferred_element_type=jnp.float32)
              + jnp.take(grad_hid, row_one, axis=0, mode='fill', fill_value=0).astype(jnp.float32)
              + jnp.take(grad_hid, row_two, axis=0, mode='fill', fill_value=0).astype(jnp.float32))
    d_ln_weight = jnp.sum(grad_h * x_hat, axis=0)
    d_ln_bias = jnp.sum(grad_h, axis=0)
    dx_tok = (dy_float + layer_norm_back(grad_h, x_hat, inv_std, ln_weight)).astype(jnp.bfloat16)
    return (out_tok, dx_tok, dw_gate, dw_up, dw_down, d_router, d_ln_weight, d_ln_bias)
```

```python
import functools

import jax
import jax.numpy as jnp
from jax import lax
from jax.experimental import pallas as pl
from jax.experimental.pallas import tpu as pltpu
from jax.sharding import PartitionSpec as P

LN_EPS = 1e-5
F32 = jnp.float32
BF16 = jnp.bfloat16
VMEM_LIMIT = 63 * 1024 * 1024
D_TILE = 1024


NT = (((1,), (1,)), ((), ()))
TN = (((0,), (0,)), ((), ()))
NN = (((1,), (0,)), ((), ()))


def mm(left, right, dims=NN):
    return lax.dot_general(left, right, dims, preferred_element_type=F32)


def build_sel(slots_ref, sel_ref):
    cap, n_tok = sel_ref.shape[1:]
    slot_ids = lax.broadcasted_iota(jnp.int32, (cap, n_tok), 0)
    for src in range(2):
        hit = slots_ref[src:src + 1, :] == slot_ids
        sel_ref[src] = jnp.where(hit, 1.0, 0.0).astype(BF16)


def fwd_body(n_k, need_o, n_prev, slots_ref, tok_a, tok_b, wg_ref, wu_ref, *refs):
    refs = list(refs)
    wd_ref = refs.pop(0) if need_o else None
    refs = refs[n_prev:]
    hb_ref, ut_ref, at_ref, bt_ref = refs[:4]
    o_refs = refs[4:6] if need_o else ()
    sel_ref = refs[-1]
    cap = sel_ref.shape[1]
    k = pl.program_id(1)

    @pl.when(k == 0)
    def _():
        build_sel(slots_ref, sel_ref)
        at_ref[...] = jnp.zeros_like(at_ref)
        bt_ref[...] = jnp.zeros_like(bt_ref)

    @pl.when(k < n_k)
    def _():
        for src, tok in enumerate((tok_a, tok_b)):
            hb_ref[src * cap:(src + 1) * cap, :] = mm(sel_ref[src], tok[...]).astype(BF16)
        at_ref[...] += mm(wg_ref[...], hb_ref[...], NT)
        bt_ref[...] += mm(wu_ref[...], hb_ref[...], NT)

    @pl.when(k == n_k - 1)
    def _():
        pre_gate = at_ref[...]
        ut_ref[...] = (pre_gate * jax.nn.sigmoid(pre_gate) * bt_ref[...]).astype(BF16)

    if need_o:
        @pl.when(k >= n_k)
        def _():
            out = mm(ut_ref[...], wd_ref[...], TN).astype(BF16)
            o_refs[0][...] = out[:cap]
            o_refs[1][...] = out[cap:]


def bwd_body(n_k, need_dh, n_prev, slots_ref, gates_ref, tok_a, tok_b, wd_ref, at_hbm, bt_hbm, *refs):
    refs = list(refs)
    if need_dh:
        wg_ref, wu_ref = refs.pop(0), refs.pop(0)
    refs = refs[n_prev:]
    qb_ref, dat_ref, dbt_ref = refs[:3]
    dh_refs = refs[3:5] if need_dh else ()
    sel_ref, g_ref, acc_ref, at_ref, bt_ref, sems = refs[-6:]
    cap = sel_ref.shape[1]
    j = pl.program_id(0)
    k = pl.program_id(1)
    copies = (pltpu.make_async_copy(at_hbm.at[j], at_ref, sems.at[0]),
              pltpu.make_async_copy(bt_hbm.at[j], bt_ref, sems.at[1]))

    @pl.when(k == 0)
    def _():
        for copy in copies:
            copy.start()
        build_sel(slots_ref, sel_ref)
        for src in range(2):
            picked = sel_ref[src].astype(F32) * gates_ref[src:src + 1, :]
            g_ref[src * cap:(src + 1) * cap, :] = jnp.sum(picked, axis=1, keepdims=True)
        acc_ref[...] = jnp.zeros_like(acc_ref)

    @pl.when(k < n_k)
    def _():
        for src, tok in enumerate((tok_a, tok_b)):
            rows = slice(src * cap, (src + 1) * cap)
            qb_ref[rows, :] = (g_ref[rows, :] * mm(sel_ref[src], tok[...])).astype(BF16)
        acc_ref[...] += mm(wd_ref[...], qb_ref[...], NT)

    @pl.when(k == n_k - 1)
    def _():
        for copy in copies:
            copy.wait()
        pre_gate = at_ref[...]
        grad_inner = acc_ref[...]
        sig = jax.nn.sigmoid(pre_gate)
        dat_ref[...] = (grad_inner * bt_ref[...] * sig * (1.0 + pre_gate * (1.0 - sig))).astype(BF16)
        dbt_ref[...] = (grad_inner * pre_gate * sig).astype(BF16)

    if need_dh:
        @pl.when(k >= n_k)
        def _():
            out = (mm(dat_ref[...], wg_ref[...], TN) + mm(dbt_ref[...], wu_ref[...], TN)).astype(BF16)
            dh_refs[0][...] = out[:cap]
            dh_refs[1][...] = out[cap:]


def dw_body(n_prev, dat_ref, dbt_ref, ut_ref, hb_ref, qb_ref, *refs):
    prev, outs = refs[:n_prev], refs[n_prev:]
    hb = hb_ref[...].reshape(-1, hb_ref.shape[-1])
    qb = qb_ref[...].reshape(-1, qb_ref.shape[-1])
    for i, (left, right) in enumerate(((dat_ref, hb), (dbt_ref, hb), (ut_ref, qb))):
        out = mm(left[...], right)
        outs[i][...] = prev[i][...] + out if n_prev else out


ANY = pl.BlockSpec(memory_space=pl.ANY)


def params(n_axes):
    return pltpu.CompilerParams(dimension_semantics=("arbitrary",) * n_axes, vmem_limit_bytes=VMEM_LIMIT)


def expert_fwd(name, slots, toks, wg, wu, wd, slot_cap, group, prev, need_o):
    n_loc, ff, d_model = wg.shape
    n_tok = toks[0].shape[0]
    rows = 2 * slot_cap
    n_k = d_model // D_TILE
    first = lambda k: jnp.minimum(k, n_k - 1)
    second = lambda k: jnp.maximum(k - n_k, 0)
    tok_spec = pl.BlockSpec((n_tok, D_TILE), lambda j, k: (0, first(k)))
    w_in = pl.BlockSpec((None, ff, D_TILE), lambda j, k: (j, 0, first(k)))
    w_out = pl.BlockSpec((None, ff, D_TILE), lambda j, k: (j, 0, second(k)))
    in_specs = [pl.BlockSpec((None, 2, n_tok), lambda j, k: (j, 0, 0)), tok_spec, tok_spec, w_in, w_in]
    args = [slots, *toks, wg, wu]
    if need_o:
        in_specs.append(w_out)
        args.append(wd)
    aliases = {}
    if prev:
        for i, arr in enumerate(prev):
            aliases[len(args)] = i
            args.append(arr)
            in_specs.append(ANY)
    out_shape = [jax.ShapeDtypeStruct((n_loc, 2, rows, d_model), BF16),
                 jax.ShapeDtypeStruct((n_loc, ff, 2 * rows), BF16),
                 jax.ShapeDtypeStruct((n_loc, ff, rows), F32),
                 jax.ShapeDtypeStruct((n_loc, ff, rows), F32)]
    out_specs = [pl.BlockSpec((None, None, rows, D_TILE), lambda j, k: (j, group, 0, first(k))),
                 pl.BlockSpec((None, ff, rows), lambda j, k: (j, 0, group)),
                 pl.BlockSpec((None, ff, rows), lambda j, k: (j, 0, 0)),
                 pl.BlockSpec((None, ff, rows), lambda j, k: (j, 0, 0))]
    if need_o:
        out_shape += [jax.ShapeDtypeStruct((n_loc, slot_cap, d_model), BF16)] * 2
        out_specs += [pl.BlockSpec((None, slot_cap, D_TILE), lambda j, k: (j, 0, second(k)))] * 2
    flops = 2 * n_loc * rows * d_model * (ff * (3 if need_o else 2) + n_tok // 2)
    return pl.pallas_call(
        functools.partial(fwd_body, n_k, need_o, len(prev or ())),
        grid=(n_loc, n_k * (2 if need_o else 1)),
        in_specs=in_specs, out_specs=out_specs, out_shape=out_shape,
        scratch_shapes=[pltpu.VMEM((2, slot_cap, n_tok), BF16)],
        input_output_aliases=aliases, compiler_params=params(2), name=name,
        cost_estimate=pl.CostEstimate(flops=flops, bytes_accessed=80 << 20, transcendentals=n_loc * ff * rows),
    )(*args)


def expert_bwd(name, slots, gates, toks, wg, wu, wd, at, bt, slot_cap, group, prev, need_dh):
    n_loc, ff, d_model = wg.shape
    n_tok = toks[0].shape[0]
    rows = 2 * slot_cap
    n_k = d_model // D_TILE
    first = lambda k: jnp.minimum(k, n_k - 1)
    second = lambda k: jnp.maximum(k - n_k, 0)
    tok_spec = pl.BlockSpec((n_tok, D_TILE), lambda j, k: (0, first(k)))
    w_in = pl.BlockSpec((None, ff, D_TILE), lambda j, k: (j, 0, first(k)))
    w_out = pl.BlockSpec((None, ff, D_TILE), lambda j, k: (j, 0, second(k)))
    tab_spec = pl.BlockSpec((None, 2, n_tok), lambda j, k: (j, 0, 0))
    in_specs = [tab_spec, tab_spec, tok_spec, tok_spec, w_in, ANY, ANY]
    args = [slots, gates, *toks, wd, at, bt]
    if need_dh:
        in_specs += [w_out, w_out]
        args += [wg, wu]
    aliases = {}
    if prev:
        for i, arr in enumerate(prev):
            aliases[len(args)] = i
            args.append(arr)
            in_specs.append(ANY)
    out_shape = [jax.ShapeDtypeStruct((n_loc, 2, rows, d_model), BF16)]
    out_shape += [jax.ShapeDtypeStruct((n_loc, ff, 2 * rows), BF16)] * 2
    out_specs = [pl.BlockSpec((None, None, rows, D_TILE), lambda j, k: (j, group, 0, first(k)))]
    out_specs += [pl.BlockSpec((None, ff, rows), lambda j, k: (j, 0, group))] * 2
    if need_dh:
        out_shape += [jax.ShapeDtypeStruct((n_loc, slot_cap, d_model), BF16)] * 2
        out_specs += [pl.BlockSpec((None, slot_cap, D_TILE), lambda j, k: (j, 0, second(k)))] * 2
    flops = 2 * n_loc * rows * d_model * (ff * (3 if need_dh else 1) + n_tok // 2)
    return pl.pallas_call(
        functools.partial(bwd_body, n_k, need_dh, len(prev or ())),
        grid=(n_loc, n_k * (2 if need_dh else 1)),
        in_specs=in_specs, out_specs=out_specs, out_shape=out_shape,
        scratch_shapes=[pltpu.VMEM((2, slot_cap, n_tok), BF16), pltpu.VMEM((rows, 1), F32),
                        pltpu.VMEM((ff, rows), F32), pltpu.VMEM((ff, rows), F32), pltpu.VMEM((ff, rows), F32),
                        pltpu.SemaphoreType.DMA((2,))],
        input_output_aliases=aliases, compiler_params=params(2), name=name,
        cost_estimate=pl.CostEstimate(flops=flops, bytes_accessed=80 << 20, transcendentals=n_loc * ff * rows),
    )(*args)


def weight_grads(name, dat, dbt, ut, hb, qb, prev):
    n_loc, ff, n_rows = dat.shape
    rows, d_model = hb.shape[2:]
    tile = 256
    left = pl.BlockSpec((None, ff, n_rows), lambda j, n: (j, 0, 0))
    right = pl.BlockSpec((None, 2, rows, tile), lambda j, n: (j, 0, 0, n))
    out = pl.BlockSpec((None, ff, tile), lambda j, n: (j, 0, n))
    prev = list(prev or ())
    return pl.pallas_call(
        functools.partial(dw_body, len(prev)),
        grid=(n_loc, d_model // tile),
        in_specs=[left] * 3 + [right] * 2 + [out] * len(prev),
        out_specs=[out] * 3,
        out_shape=[jax.ShapeDtypeStruct((n_loc, ff, d_model), F32)] * 3,
        input_output_aliases={5 + i: i for i in range(len(prev))},
        compiler_params=params(2), name=name,
        cost_estimate=pl.CostEstimate(flops=6 * n_loc * n_rows * ff * d_model, bytes_accessed=200 << 20, transcendentals=0),
    )(dat, dbt, ut, hb, qb, *prev)


def layer_norm(x_rows, ln_weight, ln_bias):
    x_float = x_rows.astype(F32)
    centered = x_float - jnp.mean(x_float, axis=-1, keepdims=True)
    inv_std = lax.rsqrt(jnp.mean(centered * centered, axis=-1, keepdims=True) + LN_EPS)
    x_hat = centered * inv_std
    hidden = (x_hat * ln_weight.astype(F32) + ln_bias.astype(F32)).astype(BF16)
    return hidden, x_hat, inv_std


def layer_norm_back(grad_h, x_hat, inv_std, ln_weight):
    scaled = grad_h * ln_weight.astype(F32)
    return inv_std * (scaled - jnp.mean(scaled, axis=-1, keepdims=True)
                      - x_hat * jnp.mean(scaled * x_hat, axis=-1, keepdims=True))


def masked_gate(logits, allowed, choice):
    expert_ids = jnp.arange(logits.shape[-1])
    prob_all = jax.nn.softmax(jnp.where(allowed, logits, -1e30), axis=-1)
    picked = (choice[:, None] == expert_ids[None, :]).astype(F32)
    return jnp.sum(prob_all * picked, axis=-1), prob_all, picked


def solution(mesh):
    n_ep = mesh.shape['ep']
    n_dp = mesh.shape['dp']
    tok_spec = P(('dp', 'ep'), None)
    row_spec = P(('dp', 'ep'))
    exp_spec = P('ep', None, None)

    def swap(arr, axis, bit):
        size = mesh.shape[axis]
        return lax.ppermute(arr, axis, [(i, i ^ bit) for i in range(size)])

    def local_step(tok_x, tok_dy, exp_first, exp_second, eligible, slot_first, slot_second,
                   ln_weight, ln_bias, router, w_gate, w_up, w_down):
        n_local, d_model = tok_x.shape
        n_exp = eligible.shape[1]
        n_loc = w_gate.shape[0]
        slot_cap = 3 * n_local // n_exp
        wg = jnp.swapaxes(w_gate, 1, 2)
        wu = jnp.swapaxes(w_up, 1, 2)
        wd = w_down
        hidden, x_hat, inv_std = layer_norm(tok_x, ln_weight, ln_bias)
        h_sib = swap(hidden, 'ep', 1)
        h_x = swap(hidden, 'ep', 2)
        h_y = swap(hidden, 'dp', 1)
        tok_dy_late, hidden = lax.optimization_barrier((tok_dy, hidden))
        dy_sib = swap(tok_dy_late, 'ep', 1)
        dy_x = swap(tok_dy_late, 'ep', 2)
        dy_y = swap(tok_dy_late, 'dp', 1)
        h_xs = swap(h_x, 'ep', 1)
        dy_xs = swap(dy_x, 'ep', 1)
        h_ys = swap(h_y, 'ep', 1)
        dy_ys = swap(dy_y, 'ep', 1)
        h_yx = swap(h_x, 'dp', 1)
        dy_yx = swap(dy_x, 'dp', 1)
        h_yxs = swap(h_yx, 'ep', 1)
        dy_yxs = swap(dy_yx, 'ep', 1)

        logits = jnp.dot(hidden, router, preferred_element_type=F32)
        expert_ids = jnp.arange(n_exp)
        allowed = eligible > 0
        gate_one, prob_one, pick_one = masked_gate(logits, allowed, exp_first)
        gate_two, prob_two, pick_two = masked_gate(logits, allowed & (expert_ids[None, :] != exp_first[:, None]), exp_second)
        pos_one = jnp.where(slot_first >= 0, exp_first * slot_cap + slot_first, -1)
        pos_two = jnp.where(slot_second >= 0, exp_second * slot_cap + slot_second, -1)
        meta = jnp.stack([pos_one.astype(F32), pos_two.astype(F32), gate_one, gate_two])
        meta_all = lax.all_gather(meta, ('dp', 'ep'))
        me = lax.axis_index('dp') * n_ep + lax.axis_index('ep')
        meta_rel = jnp.take(meta_all, me ^ jnp.arange(n_dp * n_ep), axis=0)
        first_row = ((lax.axis_index('ep') * n_loc + jnp.arange(n_loc)) * slot_cap).astype(F32)[:, None, None]
        off_one = meta_rel[None, :, 0] - first_row
        off_two = meta_rel[None, :, 1] - first_row
        in_one = (off_one >= 0) & (off_one < slot_cap)
        in_two = (off_two >= 0) & (off_two < slot_cap)
        slots = jnp.where(in_one, off_one, jnp.where(in_two, off_two, -1.0)).astype(jnp.int32)
        gates = jnp.where(in_one, meta_rel[None, :, 2], jnp.where(in_two, meta_rel[None, :, 3], 0.0))
        tabs = [(slots[:, 2 * i:2 * i + 2], gates[:, 2 * i:2 * i + 2]) for i in range(4)]

        def fwd(name, grp, toks, prev, need_o):
            return expert_fwd(name, tabs[grp][0], toks, wg, wu, wd, slot_cap, grp % 2, prev, need_o)

        def bwd(name, grp, toks, at, bt, prev, need_dh):
            return expert_bwd(name, *tabs[grp], toks, wg, wu, wd, at, bt, slot_cap, grp % 2, prev, need_dh)

        hb_a, ut_a, at0, bt0, o_own, o_sib = fwd('fwd_local', 0, (hidden, h_sib), None, True)
        qb_a, dat_a, dbt_a, dh_own, dh_sib = bwd('bwd_local', 0, (tok_dy, dy_sib), at0, bt0, None, True)
        hb_a, ut_a, at1, bt1, o_x, o_xs = fwd('fwd_x', 1, (h_x, h_xs), (hb_a, ut_a), True)
        hb_b, ut_b, at2, bt2 = fwd('fwd_y', 2, (h_y, h_ys), None, False)
        qb_a, dat_a, dbt_a, dh_x, dh_xs = bwd('bwd_x', 1, (dy_x, dy_xs), at1, bt1, (qb_a, dat_a, dbt_a), True)
        qb_b, dat_b, dbt_b = bwd('bwd_y', 2, (dy_y, dy_ys), at2, bt2, None, False)
        grads = weight_grads('dw_a', dat_a, dbt_a, ut_a, hb_a, qb_a, None)
        hb_b, ut_b, at3, bt3 = fwd('fwd_yx', 3, (h_yx, h_yxs), (hb_b, ut_b), False)
        qb_b, dat_b, dbt_b = bwd('bwd_yx', 3, (dy_yx, dy_yxs), at3, bt3, (qb_b, dat_b, dbt_b), False)
        dwg, dwu, dwd = weight_grads('dw_b', dat_b, dbt_b, ut_b, hb_b, qb_b, grads)

        def bring_back(own, sib, same, cross):
            return jnp.concatenate([own, swap(sib, 'ep', 1), swap(same, 'ep', 2), swap(cross, 'ep', 3)]).reshape(
                n_exp * slot_cap, d_model)

        out_back = bring_back(o_own, o_sib, o_x, o_xs)
        hid_back = bring_back(dh_own, dh_sib, dh_x, dh_xs)
        ep_me = lax.axis_index('ep')

        def selector(expert, slot):
            rel = (expert // n_loc) ^ ep_me
            pos = jnp.where(slot >= 0, (rel * n_loc + expert % n_loc) * slot_cap + slot, -1)
            return (pos[:, None] == jnp.arange(n_exp * slot_cap)[None, :]).astype(BF16)

        sel_one = selector(exp_first, slot_first)
        sel_two = selector(exp_second, slot_second)
        out_one = jnp.dot(sel_one, out_back, preferred_element_type=F32)
        out_two = jnp.dot(sel_two, out_back, preferred_element_type=F32)
        y_mix = gate_one[:, None] * out_one + gate_two[:, None] * out_two
        out_tok = (tok_x.astype(F32) + y_mix).astype(BF16)
        dy_float = tok_dy.astype(F32)
        grad_exp = jnp.dot(sel_one + sel_two, hid_back, preferred_element_type=F32)
        dgate_one = jnp.sum(dy_float * out_one, axis=-1)
        dgate_two = jnp.sum(dy_float * out_two, axis=-1)
        d_logits = ((dgate_one * gate_one)[:, None] * (pick_one - prob_one)
                    + (dgate_two * gate_two)[:, None] * (pick_two - prob_two)).astype(BF16)
        d_router = jnp.einsum('td,te->de', hidden, d_logits, preferred_element_type=F32)
        grad_h = jnp.einsum('te,de->td', d_logits, router, preferred_element_type=F32) + grad_exp
        d_ln_weight = jnp.sum(grad_h * x_hat, axis=0)
        d_ln_bias = jnp.sum(grad_h, axis=0)
        dx_tok = (dy_float + layer_norm_back(grad_h, x_hat, inv_std, ln_weight)).astype(BF16)
        d_router = lax.psum(d_router, ('dp', 'ep'))
        d_ln_weight = lax.psum(d_ln_weight, ('dp', 'ep'))
        d_ln_bias = lax.psum(d_ln_bias, ('dp', 'ep'))
        return (out_tok, dx_tok, jnp.swapaxes(dwg, 1, 2), jnp.swapaxes(dwu, 1, 2), dwd,
                d_router, d_ln_weight, d_ln_bias)

    return jax.shard_map(
        local_step, mesh=mesh,
        in_specs=(tok_spec, tok_spec, row_spec, row_spec, tok_spec, row_spec, row_spec,
                  P(), P(), P(), exp_spec, exp_spec, exp_spec),
        out_specs=(tok_spec, tok_spec, exp_spec, exp_spec, exp_spec, P(), P(), P()),
        check_vma=False)
```

```python
import functools

import jax
import jax.numpy as jnp
from jax import lax
from jax.experimental import pallas as pl
from jax.experimental.pallas import tpu as pltpu
from jax.sharding import PartitionSpec as P


LN_EPS = 1e-5
F32 = jnp.float32
BF16 = jnp.bfloat16
VMEM_LIMIT = 63 * 1024 * 1024
D_TILE = 1024
ROW_TILE = 128
COL_TILE = 512
NEG = -1e30


NN = (((1,), (0,)), ((), ()))
NT = (((1,), (1,)), ((), ()))
TN = (((0,), (0,)), ((), ()))

POS_ONE, POS_TWO, GATE_ONE, GATE_TWO, REL_ONE, REL_TWO, MEAN, INV_STD = range(8)

ANY = pl.BlockSpec(memory_space=pl.ANY)
SMEM = pl.BlockSpec(memory_space=pltpu.SMEM)


def mm(left, right, dims=NN):
    return lax.dot_general(left, right, dims, preferred_element_type=F32)


def params(n_axes):
    return pltpu.CompilerParams(dimension_semantics=("arbitrary",) * n_axes, vmem_limit_bytes=VMEM_LIMIT)


def cost(flops, n_bytes, transcendentals=0):
    return pl.CostEstimate(flops=int(flops), bytes_accessed=int(n_bytes), transcendentals=int(transcendentals))


def front_body(n_loc, slot_cap, ep_ref, x_ref, norm_ref, router_ref, first_ref, second_ref, elig_ref,
               slot_one_ref, slot_two_ref, h_ref, meta_ref, cols_ref, diff_one_ref, diff_two_ref):
    x_float = x_ref[...].astype(F32)
    mean = jnp.mean(x_float, axis=-1, keepdims=True)
    centered = x_float - mean
    inv_std = lax.rsqrt(jnp.mean(centered * centered, axis=-1, keepdims=True) + LN_EPS)
    hidden = (centered * inv_std * norm_ref[0:1, :] + norm_ref[1:2, :]).astype(BF16)
    h_ref[...] = hidden
    n_row = x_float.shape[0]
    n_exp = elig_ref.shape[0]
    logits = jnp.concatenate([mm(hidden, router_ref[...], NT), jnp.zeros((n_row, n_row - n_exp), F32)], axis=1).T[:n_exp]
    ids = lax.broadcasted_iota(jnp.int32, (n_exp, n_row), 0)
    first, second = first_ref[...], second_ref[...]
    pick_one = ids == first
    pick_two = ids == second
    allowed = elig_ref[...] > 0
    tabs = []
    for mask, pick in ((allowed, pick_one), (allowed & jnp.logical_not(pick_one), pick_two)):
        masked = jnp.where(mask, logits, NEG)
        powers = jnp.exp(masked - jnp.max(masked, axis=0, keepdims=True))
        prob = powers / jnp.sum(powers, axis=0, keepdims=True)
        hot = jnp.where(pick, 1.0, 0.0)
        tabs.append((jnp.sum(prob * hot, axis=0, keepdims=True), hot - prob))
    rows = []
    for expert, slot in ((first, slot_one_ref[...]), (second, slot_two_ref[...])):
        rows.append(jnp.where(slot >= 0, expert * slot_cap + slot, -1).astype(F32))
    rows += [tabs[0][0], tabs[1][0]]
    for expert, slot in ((first, slot_one_ref[...]), (second, slot_two_ref[...])):
        block = expert ^ (ep_ref[0] * n_loc)
        rows.append(jnp.where(slot >= 0, block * slot_cap + slot, -1).astype(F32))
    rows += [jnp.zeros_like(rows[0])] * 2
    meta = jnp.concatenate(rows, axis=0)
    meta_ref[...] = meta
    fill = jnp.zeros((n_row - n_exp, n_row), F32)
    lanes = lax.broadcasted_iota(jnp.int32, (n_row, n_row), 1)
    cols = jnp.concatenate([meta, fill], axis=0).T
    cols_ref[...] = jnp.where(lanes == MEAN, mean, jnp.where(lanes == INV_STD, inv_std, cols))
    diff_one_ref[...] = jnp.concatenate([tabs[0][1], fill], axis=0).T
    diff_two_ref[...] = jnp.concatenate([tabs[1][1], fill], axis=0).T


def front(ep, tok_x, norm, router_rows, first, second, elig, slot_one, slot_two, n_loc, slot_cap):
    n_tok, d_model = tok_x.shape
    n_exp = elig.shape[0]
    row = pl.BlockSpec((ROW_TILE, d_model), lambda i: (i, 0))
    tab = lambda n: pl.BlockSpec((n, ROW_TILE), lambda i: (0, i))
    col = pl.BlockSpec((ROW_TILE, 128), lambda i: (i, 0))
    wide = jax.ShapeDtypeStruct((n_tok, 128), F32)
    return pl.pallas_call(
        functools.partial(front_body, n_loc, slot_cap),
        grid=(n_tok // ROW_TILE,),
        in_specs=[SMEM, row, pl.BlockSpec(norm.shape, lambda i: (0, 0)), pl.BlockSpec(router_rows.shape, lambda i: (0, 0)),
                  tab(1), tab(1), tab(n_exp), tab(1), tab(1)],
        out_specs=[row, tab(8), col, col, col],
        out_shape=[jax.ShapeDtypeStruct((n_tok, d_model), BF16), jax.ShapeDtypeStruct((8, n_tok), F32), wide, wide, wide],
        compiler_params=params(1), name="front", cost_estimate=cost(2 * n_tok * d_model * 128, 4 * n_tok * d_model),
    )(ep, tok_x, norm, router_rows, first[None], second[None], elig, slot_one[None],
      slot_two[None])


def pick_slots(meta_ref, expert, slot_cap):
    first_row = (expert * slot_cap).astype(F32)
    off_one = meta_ref[POS_ONE:POS_ONE + 1, :] - first_row
    off_two = meta_ref[POS_TWO:POS_TWO + 1, :] - first_row
    in_one = (off_one >= 0) & (off_one < slot_cap)
    in_two = (off_two >= 0) & (off_two < slot_cap)
    slot = jnp.where(in_one, off_one, jnp.where(in_two, off_two, -1.0))
    gate = jnp.where(in_one, meta_ref[GATE_ONE:GATE_ONE + 1, :],
                     jnp.where(in_two, meta_ref[GATE_TWO:GATE_TWO + 1, :], 0.0))
    return slot.astype(jnp.int32), gate


def build_sel(metas, expert, sel_ref, g_ref=None):
    cap, n_tok = sel_ref.shape[1:]
    slot_ids = lax.broadcasted_iota(jnp.int32, (cap, n_tok), 0)
    for src, meta_ref in enumerate(metas):
        slot, gate = pick_slots(meta_ref, expert, cap)
        hit = slot == slot_ids
        sel_ref[src] = jnp.where(hit, 1.0, 0.0).astype(BF16)
        if g_ref is not None:
            g_ref[src * cap:(src + 1) * cap, :] = jnp.sum(jnp.where(hit, gate, 0.0), axis=1, keepdims=True)


def fwd_body(n_k, n_loc, need_o, n_skip, ep_ref, meta_a, meta_b, tok_a, tok_b, wg_ref, wu_ref, *refs):
    refs = list(refs)
    wd_ref = refs.pop(0) if need_o else None
    refs = refs[n_skip:]
    hb_ref, ut_ref, pt_ref, qt_ref = refs[:4]
    o_refs = refs[4:6] if need_o else ()
    sel_ref = refs[-1]
    cap = sel_ref.shape[1]
    k = pl.program_id(1)

    @pl.when(k == 0)
    def _():
        build_sel((meta_a, meta_b), ep_ref[0] * n_loc + pl.program_id(0), sel_ref)

    def gather():
        for src, tok in enumerate((tok_a, tok_b)):
            hb_ref[src * cap:(src + 1) * cap, :] = mm(sel_ref[src], tok[...]).astype(BF16)

    @pl.when(k < n_k - 1)
    def _():
        gather()
        fresh = k == 0
        pt_ref[...] = jnp.where(fresh, 0.0, pt_ref[...]) + mm(wg_ref[...], hb_ref[...], NT)
        qt_ref[...] = jnp.where(fresh, 0.0, qt_ref[...]) + mm(wu_ref[...], hb_ref[...], NT)

    @pl.when(k == n_k - 1)
    def _():
        gather()
        rows = pt_ref.shape[1]
        for c in range(0, rows, 256):
            part = slice(c, c + 256)
            pre_gate = pt_ref[:, part] + mm(wg_ref[...], hb_ref[part, :], NT)
            pre_up = qt_ref[:, part] + mm(wu_ref[...], hb_ref[part, :], NT)
            sig = jax.nn.sigmoid(pre_gate)
            silu = pre_gate * sig
            ut_ref[:, part] = (silu * pre_up).astype(BF16)
            pt_ref[:, part] = pre_up * (sig * (1.0 + pre_gate * (1.0 - sig)))
            qt_ref[:, part] = silu

    if need_o:
        @pl.when(k >= n_k)
        def _():
            out = mm(ut_ref[...], wd_ref[...], TN).astype(BF16)
            o_refs[0][...] = out[:cap]
            o_refs[1][...] = out[cap:]


def bwd_body(n_k, n_loc, need_dh, n_skip, ep_ref, meta_a, meta_b, tok_a, tok_b, wd_ref, pt_hbm, qt_hbm, *refs):
    refs = list(refs)
    if need_dh:
        wg_ref, wu_ref = refs.pop(0), refs.pop(0)
    refs = refs[n_skip:]
    qb_ref, dat_ref, dbt_ref = refs[:3]
    dh_refs = refs[3:5] if need_dh else ()
    sel_ref, g_ref, acc_ref, pt_ref, qt_ref, sems = refs[-6:]
    cap = sel_ref.shape[1]
    j = pl.program_id(0)
    k = pl.program_id(1)
    copies = (pltpu.make_async_copy(pt_hbm.at[j], pt_ref, sems.at[0]),
              pltpu.make_async_copy(qt_hbm.at[j], qt_ref, sems.at[1]))

    @pl.when(k == 0)
    def _():
        for copy in copies:
            copy.start()
        build_sel((meta_a, meta_b), ep_ref[0] * n_loc + j, sel_ref, g_ref)

    def gather():
        for src, tok in enumerate((tok_a, tok_b)):
            rows = slice(src * cap, (src + 1) * cap)
            qb_ref[rows, :] = (g_ref[rows, :] * mm(sel_ref[src], tok[...])).astype(BF16)

    @pl.when(k < n_k - 1)
    def _():
        gather()
        acc_ref[...] = jnp.where(k == 0, 0.0, acc_ref[...]) + mm(wd_ref[...], qb_ref[...], NT)

    @pl.when(k == n_k - 1)
    def _():
        for copy in copies:
            copy.wait()
        gather()
        for c in range(0, acc_ref.shape[1], 256):
            part = slice(c, c + 256)
            grad_inner = acc_ref[:, part] + mm(wd_ref[...], qb_ref[part, :], NT)
            dat_ref[:, part] = (grad_inner * pt_ref[:, part]).astype(BF16)
            dbt_ref[:, part] = (grad_inner * qt_ref[:, part]).astype(BF16)

    if need_dh:
        @pl.when(k >= n_k)
        def _():
            out = (mm(dat_ref[...], wg_ref[...], TN) + mm(dbt_ref[...], wu_ref[...], TN)).astype(BF16)
            dh_refs[0][...] = out[:cap]
            dh_refs[1][...] = out[cap:]


def expert_specs(wg, slot_cap, n_tok):
    ff, d_model = wg.shape[1:]
    n_k = d_model // D_TILE
    first = lambda k: jnp.minimum(k, n_k - 1)
    second = lambda k: jnp.maximum(k - n_k, 0)
    meta = pl.BlockSpec((8, n_tok), lambda j, k: (0, 0))
    tok = pl.BlockSpec((n_tok, D_TILE), lambda j, k: (0, first(k)))
    w_in = pl.BlockSpec((None, ff, D_TILE), lambda j, k: (j, 0, first(k)))
    w_out = pl.BlockSpec((None, ff, D_TILE), lambda j, k: (j, 0, second(k)))
    back = pl.BlockSpec((None, slot_cap, D_TILE), lambda j, k: (j, 0, second(k)))
    return n_k, first, meta, tok, w_in, w_out, back


def expert_fwd(ep, metas, toks, wg, wu, wd, slot_cap, group, prev, need_o, deps):
    n_loc, ff, d_model = wg.shape
    n_tok = toks[0].shape[0]
    rows = 2 * slot_cap
    n_k, first, meta, tok, w_in, w_out, back = expert_specs(wg, slot_cap, n_tok)
    in_specs = [SMEM, meta, meta, tok, tok, w_in, w_in]
    args = [ep, *metas, *toks, wg, wu]
    if need_o:
        in_specs.append(w_out)
        args.append(wd)
    aliases = {len(args) + i: i for i in range(len(prev))}
    args += [*prev, *deps]
    in_specs += [ANY] * (len(prev) + len(deps))
    act = pl.BlockSpec((None, ff, rows), lambda j, k: (j, 0, 0))
    out_shape = [jax.ShapeDtypeStruct((n_loc, 2, rows, d_model), BF16),
                 jax.ShapeDtypeStruct((n_loc, ff, 2 * rows), BF16)]
    out_shape += [jax.ShapeDtypeStruct((n_loc, ff, rows), F32)] * 2
    out_specs = [pl.BlockSpec((None, None, rows, D_TILE), lambda j, k: (j, group, 0, first(k))),
                 pl.BlockSpec((None, ff, rows), lambda j, k: (j, 0, group)), act, act]
    if need_o:
        out_shape += [jax.ShapeDtypeStruct((n_loc, slot_cap, d_model), BF16)] * 2
        out_specs += [back] * 2
    flops = 2 * n_loc * rows * d_model * (ff * (3 if need_o else 2) + n_tok)
    return pl.pallas_call(
        functools.partial(fwd_body, n_k, n_loc, need_o, len(prev) + len(deps)),
        grid=(n_loc, n_k * (2 if need_o else 1)),
        in_specs=in_specs, out_specs=out_specs, out_shape=out_shape,
        scratch_shapes=[pltpu.VMEM((2, slot_cap, n_tok), BF16)],
        input_output_aliases=aliases, compiler_params=params(2),
        cost_estimate=cost(flops, 80e6, n_loc * ff * rows),
    )(*args)


def expert_bwd(ep, metas, toks, wg, wu, wd, pt, qt, slot_cap, group, prev, need_dh, deps):
    n_loc, ff, d_model = wg.shape
    n_tok = toks[0].shape[0]
    rows = 2 * slot_cap
    n_k, first, meta, tok, w_in, w_out, back = expert_specs(wg, slot_cap, n_tok)
    in_specs = [SMEM, meta, meta, tok, tok, w_in, ANY, ANY]
    args = [ep, *metas, *toks, wd, pt, qt]
    if need_dh:
        in_specs += [w_out, w_out]
        args += [wg, wu]
    aliases = {len(args) + i: i for i in range(len(prev))}
    args += [*prev, *deps]
    in_specs += [ANY] * (len(prev) + len(deps))
    out_shape = [jax.ShapeDtypeStruct((n_loc, 2, rows, d_model), BF16)]
    out_shape += [jax.ShapeDtypeStruct((n_loc, ff, 2 * rows), BF16)] * 2
    out_specs = [pl.BlockSpec((None, None, rows, D_TILE), lambda j, k: (j, group, 0, first(k)))]
    out_specs += [pl.BlockSpec((None, ff, rows), lambda j, k: (j, 0, group))] * 2
    if need_dh:
        out_shape += [jax.ShapeDtypeStruct((n_loc, slot_cap, d_model), BF16)] * 2
        out_specs += [back] * 2
    flops = 2 * n_loc * rows * d_model * (ff * (3 if need_dh else 1) + n_tok)
    act = pltpu.VMEM((ff, rows), F32)
    return pl.pallas_call(
        functools.partial(bwd_body, n_k, n_loc, need_dh, len(prev) + len(deps)),
        grid=(n_loc, n_k * (2 if need_dh else 1)),
        in_specs=in_specs, out_specs=out_specs, out_shape=out_shape,
        scratch_shapes=[pltpu.VMEM((2, slot_cap, n_tok), BF16), pltpu.VMEM((rows, 1), F32), act, act, act,
                        pltpu.SemaphoreType.DMA((2,))],
        input_output_aliases=aliases, compiler_params=params(2),
        cost_estimate=cost(flops, 80e6),
    )(*args)


def dw_body(n_prev, n_skip, dat_ref, dbt_ref, ut_ref, hb_ref, qb_ref, *refs):
    prev, outs = refs[:n_prev], refs[n_prev + n_skip:]
    hb = hb_ref[...].reshape(-1, hb_ref.shape[-1])
    qb = qb_ref[...].reshape(-1, qb_ref.shape[-1])
    for i, (left, right) in enumerate(((dat_ref, hb), (dbt_ref, hb), (ut_ref, qb))):
        out = mm(left[...], right)
        outs[i][...] = prev[i][...] + out if n_prev else out


def weight_grads(dat, dbt, ut, hb, qb, prev, deps):
    n_loc, ff, n_rows = dat.shape
    rows, d_model = hb.shape[2:]
    tile = 256
    left = pl.BlockSpec((None, ff, n_rows), lambda j, n: (j, 0, 0))
    right = pl.BlockSpec((None, 2, rows, tile), lambda j, n: (j, 0, 0, n))
    out = pl.BlockSpec((None, ff, tile), lambda j, n: (j, 0, n))
    return pl.pallas_call(
        functools.partial(dw_body, len(prev), len(deps)),
        grid=(n_loc, d_model // tile),
        in_specs=[left] * 3 + [right] * 2 + [out] * len(prev) + [ANY] * len(deps),
        out_specs=[out] * 3,
        out_shape=[jax.ShapeDtypeStruct((n_loc, ff, d_model), F32)] * 3,
        input_output_aliases={5 + i: i for i in range(len(prev))},
        compiler_params=params(2), cost_estimate=cost(6 * n_loc * n_rows * ff * d_model, 200e6),
    )(dat, dbt, ut, hb, qb, *prev, *deps)


def fold(values):
    total = values[:, :128]
    for c in range(128, values.shape[1], 128):
        total = total + values[:, c:c + 128]
    return total


def one_hot(cols_ref, which, n_slot):
    n_tok = cols_ref.shape[0]
    ids = lax.broadcasted_iota(jnp.int32, (n_tok, n_slot), 1)
    return ids == cols_ref[:, which:which + 1].astype(jnp.int32)


def mix_body(n_col, n_skip, cols_ref, diff_one_ref, diff_two_ref, x_ref, dy_ref, h_ref, *refs):
    blocks = refs[:4]
    out_ref, s_ref, dr_ref, sel_ref, dot_ref, st_ref = refs[4 + n_skip:]
    i = pl.program_id(0)
    n_tok = x_ref.shape[0]

    @pl.when(i == 0)
    def _():
        for k, which in enumerate((REL_ONE, REL_TWO)):
            sel_ref[k] = jnp.where(one_hot(cols_ref, which, sel_ref.shape[2]), 1.0, 0.0).astype(BF16)
        dot_ref[...] = jnp.zeros_like(dot_ref)

    @pl.when(i < n_col)
    def _():
        parts = [blk[...].reshape(-1, blk.shape[-1]) for blk in blocks]
        n_part = parts[0].shape[0]
        half = n_tok // 2
        for r in range(0, n_tok, half):
            rows = slice(r, r + half)
            dy_float = dy_ref[rows, :].astype(F32)
            mixed = x_ref[rows, :].astype(F32)
            for k, gate in enumerate((GATE_ONE, GATE_TWO)):
                out = mm(sel_ref[k, rows, :n_part], parts[0])
                for b in range(1, 4):
                    out = out + mm(sel_ref[k, rows, b * n_part:(b + 1) * n_part], parts[b])
                dot_ref[k, rows, :] += fold(dy_float * out)
                mixed = mixed + cols_ref[rows, gate:gate + 1] * out
            out_ref[rows, :] = mixed.astype(BF16)

    @pl.when(i == n_col)
    def _():
        total = jnp.zeros(diff_one_ref.shape, F32)
        for k, (gate, diff) in enumerate(((GATE_ONE, diff_one_ref), (GATE_TWO, diff_two_ref))):
            scale = jnp.sum(dot_ref[k], axis=1, keepdims=True) * cols_ref[:, gate:gate + 1]
            total = total + scale * diff[...]
        s_ref[...] = total.astype(BF16)
        st_ref[...] = total.T.astype(BF16)

    @pl.when(i >= n_col)
    def _():
        dr_ref[...] = mm(st_ref[...], h_ref[...])[:dr_ref.shape[0]]


def mix(cols, diff_one, diff_two, tok_x, tok_dy, hidden, blocks, n_exp, deps):
    n_tok, d_model = tok_x.shape
    n_loc, cap, _ = blocks[0].shape
    n_col = d_model // COL_TILE
    h_tile = 2 * COL_TILE
    first = lambda i: jnp.minimum(i, n_col - 1)
    second = lambda i: jnp.maximum(i - n_col, 0)
    whole = pl.BlockSpec((n_tok, 128), lambda i: (0, 0))
    tile = pl.BlockSpec((n_tok, COL_TILE), lambda i: (0, first(i)))
    block = pl.BlockSpec((n_loc, cap, COL_TILE), lambda i: (0, 0, first(i)))
    n_slot = 4 * n_loc * cap
    return pl.pallas_call(
        functools.partial(mix_body, n_col, len(deps)),
        grid=(n_col + d_model // h_tile,),
        in_specs=[whole] * 3 + [tile] * 2 + [pl.BlockSpec((n_tok, h_tile), lambda i: (0, second(i)))] + [block] * 4
        + [ANY] * len(deps),
        out_specs=[tile, whole, pl.BlockSpec((n_exp, h_tile), lambda i: (0, second(i)))],
        out_shape=[jax.ShapeDtypeStruct((n_tok, d_model), BF16), jax.ShapeDtypeStruct((n_tok, 128), BF16),
                   jax.ShapeDtypeStruct((n_exp, d_model), F32)],
        scratch_shapes=[pltpu.VMEM((2, n_tok, n_slot), BF16), pltpu.VMEM((2, n_tok, 128), F32),
                        pltpu.VMEM((128, n_tok), BF16)],
        compiler_params=params(1), name="mix", cost_estimate=cost(4 * n_tok * n_slot * d_model, 60e6),
    )(cols, diff_one, diff_two, tok_x, tok_dy, hidden, *blocks, *deps)


def tail_body(n_col, n_skip, cols_ref, s_ref, x_ref, dy_ref, norm_ref, router_ref, *refs):
    blocks = refs[:4]
    dx_ref, sums_ref, sel_ref, gh_ref, dot_ref = refs[4 + n_skip:]
    i = pl.program_id(0)
    n_tok, tile = x_ref.shape
    d_model = n_col * tile

    @pl.when(i == 0)
    def _():
        hit = one_hot(cols_ref, REL_ONE, sel_ref.shape[1]) | one_hot(cols_ref, REL_TWO, sel_ref.shape[1])
        sel_ref[...] = jnp.where(hit, 1.0, 0.0).astype(BF16)
        dot_ref[...] = jnp.zeros_like(dot_ref)

    half = n_tok // 2

    def x_hat(rows):
        return (x_ref[rows, :].astype(F32) - cols_ref[rows, MEAN:MEAN + 1]) * cols_ref[rows, INV_STD:INV_STD + 1]

    @pl.when(i < n_col)
    def _():
        parts = [blk[...].reshape(-1, blk.shape[-1]) for blk in blocks]
        n_part = parts[0].shape[0]
        d_bias = jnp.zeros((1, tile), F32)
        d_weight = jnp.zeros((1, tile), F32)
        for r in range(0, n_tok, half):
            rows = slice(r, r + half)
            grad_h = mm(s_ref[rows, :router_ref.shape[0]], router_ref[...])
            for b in range(4):
                grad_h = grad_h + mm(sel_ref[rows, b * n_part:(b + 1) * n_part], parts[b])
            gh_ref[i, rows, :] = grad_h
            normed = x_hat(rows)
            product = grad_h * normed
            weight = norm_ref[0:1, :]
            dot_ref[0, rows, :] += fold(grad_h * weight)
            dot_ref[1, rows, :] += fold(product * weight)
            d_bias = d_bias + jnp.sum(grad_h, axis=0, keepdims=True)
            d_weight = d_weight + jnp.sum(product, axis=0, keepdims=True)
        sums_ref[0:1, :] = d_weight
        sums_ref[1:2, :] = d_bias

    @pl.when(i == n_col)
    def _():
        for k in range(2):
            total = jnp.sum(dot_ref[k], axis=1, keepdims=True) * (1.0 / d_model)
            dot_ref[k] = jnp.broadcast_to(total, dot_ref.shape[1:])

    @pl.when(i >= n_col)
    def _():
        for r in range(0, n_tok, half):
            rows = slice(r, r + half)
            scaled = gh_ref[i - n_col, rows, :] * norm_ref[0:1, :]
            back = scaled - dot_ref[0, rows, 0:1] - x_hat(rows) * dot_ref[1, rows, 0:1]
            grad = dy_ref[rows, :].astype(F32) + cols_ref[rows, INV_STD:INV_STD + 1] * back
            dx_ref[rows, :] = grad.astype(BF16)


def tail(cols, s_rows, tok_x, tok_dy, norm, router_rows, blocks, deps):
    n_tok, d_model = tok_x.shape
    n_loc, cap, _ = blocks[0].shape
    n_col = d_model // COL_TILE
    first = lambda i: jnp.minimum(i, n_col - 1)
    second = lambda i: jnp.maximum(i - n_col, 0)
    both = lambda i: lax.rem(i, n_col)
    whole = pl.BlockSpec((n_tok, 128), lambda i: (0, 0))
    block = pl.BlockSpec((n_loc, cap, COL_TILE), lambda i: (0, 0, first(i)))
    n_slot = 4 * n_loc * cap
    return pl.pallas_call(
        functools.partial(tail_body, n_col, len(deps)),
        grid=(2 * n_col,),
        in_specs=[whole, whole, pl.BlockSpec((n_tok, COL_TILE), lambda i: (0, both(i))),
                  pl.BlockSpec((n_tok, COL_TILE), lambda i: (0, second(i))),
                  pl.BlockSpec((2, COL_TILE), lambda i: (0, both(i))),
                  pl.BlockSpec((router_rows.shape[0], COL_TILE), lambda i: (0, first(i)))] + [block] * 4 + [ANY] * len(deps),
        out_specs=[pl.BlockSpec((n_tok, COL_TILE), lambda i: (0, second(i))),
                   pl.BlockSpec((2, COL_TILE), lambda i: (0, first(i)))],
        out_shape=[jax.ShapeDtypeStruct((n_tok, d_model), BF16), jax.ShapeDtypeStruct((2, d_model), F32)],
        scratch_shapes=[pltpu.VMEM((n_tok, n_slot), BF16), pltpu.VMEM((n_col, n_tok, COL_TILE), F32),
                        pltpu.VMEM((2, n_tok, 128), F32)],
        compiler_params=params(1), name="tail", cost_estimate=cost(2 * n_tok * n_slot * d_model, 60e6),
    )(cols, s_rows, tok_x, tok_dy, norm, router_rows, *blocks, *deps)


def solution(mesh):
    n_ep = mesh.shape['ep']
    n_dp = mesh.shape['dp']
    n_dev = n_ep * n_dp
    tok_spec = P(('dp', 'ep'), None)
    row_spec = P(('dp', 'ep'))
    exp_spec = P('ep', None, None)
    route = {"sib": 1, "x": 2, "xs": 3, "y": n_ep, "ys": n_ep + 1, "yx": n_ep + 2, "yxs": n_ep + 3}

    def swap(arr, way):
        return lax.ppermute(arr, ('dp', 'ep'), [(i, i ^ route[way]) for i in range(n_dev)])

    def after(arr, done):
        return lax.optimization_barrier((arr, done))[0]

    def step(tok_x, tok_dy, exp_first, exp_second, eligible, slot_first, slot_second,
             ln_weight, ln_bias, router, w_gate, w_up, w_down):
        n_local, _ = tok_x.shape
        n_exp = eligible.shape[1]
        n_loc = w_gate.shape[0]
        slot_cap = 3 * n_local // n_exp
        wg = jnp.swapaxes(w_gate, 1, 2)
        wu = jnp.swapaxes(w_up, 1, 2)
        ep = lax.axis_index('ep').astype(jnp.int32)[None]
        router_rows = router.T
        norm = jnp.stack([ln_weight, ln_bias]).astype(F32)
        hidden, meta, cols, diff_one, diff_two = front(
            ep, tok_x, norm, router_rows, exp_first, exp_second, eligible.T, slot_first, slot_second, n_loc, slot_cap)
        metas = [meta] + [swap(meta, way) for way in route]
        h = {way: swap(hidden, way) for way in ("sib", "x", "y")}
        dy = {way: swap(tok_dy, way) for way in ("sib", "x", "y")}
        for rows in (h, dy):
            rows["xs"] = swap(rows["x"], "sib")
            rows["yx"] = swap(rows["x"], "y")
            rows["ys"] = swap(rows["y"], "sib")
            rows["yxs"] = swap(rows["yx"], "sib")

        def fwd(grp, toks, prev, need_o, deps):
            return expert_fwd(ep, metas[2 * grp:2 * grp + 2], toks, wg, wu, w_down, slot_cap, grp % 2, prev,
                              need_o, deps)

        def bwd(grp, toks, pt, qt, prev, need_dh, deps):
            return expert_bwd(ep, metas[2 * grp:2 * grp + 2], toks, wg, wu, w_down, pt, qt, slot_cap, grp % 2,
                              prev, need_dh, deps)

        hb_a, ut_a, pt0, qt0, o_own, o_sib = fwd(0, (hidden, h["sib"]), (), True, ())
        qb_a, dat_a, dbt_a, dh_own, dh_sib = bwd(0, (tok_dy, dy["sib"]), pt0, qt0, (), True, ())
        hb_a, ut_a, pt1, qt1, o_x, o_xs = fwd(1, (h["x"], h["xs"]), (hb_a, ut_a), True, (dh_own,))
        hb_b, ut_b, pt2, qt2 = fwd(2, (h["y"], h["ys"]), (), False, (pt1,))
        qb_a, dat_a, dbt_a, dh_x, dh_xs = bwd(1, (dy["x"], dy["xs"]), pt1, qt1, (qb_a, dat_a, dbt_a), True,
                                              (pt2,))
        qb_b, dat_b, dbt_b = bwd(2, (dy["y"], dy["ys"]), pt2, qt2, (), False, (qb_a,))
        grads = weight_grads(dat_a, dbt_a, ut_a, hb_a, qb_a, (), (qb_b,))
        blocks = (o_own, swap(o_sib, "sib"), swap(o_x, "x"), swap(o_xs, "xs"))
        out_tok, s_rows, d_router = mix(cols, diff_one, diff_two, tok_x, tok_dy, hidden, blocks, n_exp, (grads[0],))
        hb_b, ut_b, pt3, qt3 = fwd(3, (h["yx"], h["yxs"]), (hb_b, ut_b), False, (s_rows,))
        qb_b, dat_b, dbt_b = bwd(3, (dy["yx"], dy["yxs"]), pt3, qt3, (qb_b, dat_b, dbt_b), False, ())
        dwg, dwu, dwd = weight_grads(dat_b, dbt_b, ut_b, hb_b, qb_b, grads, ())
        blocks = (dh_own, swap(dh_sib, "sib"), swap(dh_x, "x"), swap(dh_xs, "xs"))
        dx_tok, sums = tail(cols, s_rows, tok_x, tok_dy, norm, router_rows, blocks, (dwg,))
        d_router = d_router + after(swap(d_router, "sib"), pt3)
        d_router = d_router + after(swap(d_router, "y"), dat_b)
        d_router = d_router + after(swap(d_router, "x"), sums)
        sums = jnp.sum(lax.all_gather(sums, ('dp', 'ep')), axis=0)
        return (out_tok, dx_tok, jnp.swapaxes(dwg, 1, 2), jnp.swapaxes(dwu, 1, 2), dwd,
                d_router.T, sums[0], sums[1])

    return jax.shard_map(
        step, mesh=mesh,
        in_specs=(tok_spec, tok_spec, row_spec, row_spec, tok_spec, row_spec, row_spec,
                  P(), P(), P(), exp_spec, exp_spec, exp_spec),
        out_specs=(tok_spec, tok_spec, exp_spec, exp_spec, exp_spec, P(), P(), P()),
        check_vma=False)
```
